8 devices in a mesh: dp: 2 (over y, z), sp: 4 (over x, core).
Axes of the slice: x: 2, y: 2, z: 1, core: 2. Of those that a mesh axis runs over, the one named last changes fastest.
Arguments:
- x: bfloat16 [2048, 7168], P(('dp', 'sp')), parts along dimension 0
- gain: bfloat16 [7168], replicated
- wq: bfloat16 [7168, 7168], replicated
- wk: bfloat16 [7168, 7168], replicated
- wv: bfloat16 [7168, 7168], replicated
- wo: bfloat16 [7168, 7168], replicated
Outputs:
- output: bfloat16 [2048, 7168], P(('dp', 'sp')), parts along dimension 0
There are 2 independent parts. The reference program is written for one: setup_inputs(seed, part) draws one part's arguments, and reference() takes and returns one part's arrays. A program takes and returns all parts, laid end to end along the dimension named above; an argument that names none is the same for every part.
All inputs are finite; a program needn't handle non-finite values.
Results may differ from the reference program's by a relative error of at most 0.012.
Values are sent between devices in bfloat16 or wider.
A program may use at most 2 GiB of HBM per device.

```python
import jax
import jax.numpy as jnp
from jax import lax

ROWS = 1024
D = 7168
HEADS = 56
KV_HEADS = 56
HEAD = 128
THETA = 10000


def setup_inputs(seed: int = 0, part: int = 0) -> dict:
    kx, kn, kq, kk, kv, ko = jax.random.split(jax.random.key(seed), 6)

    def weights(key, rows, columns):
        return jax.random.normal(key, (rows, columns), jnp.float32) * rows**-0.5

    drawn = {
        "x": jax.random.normal(jax.random.fold_in(kx, part), (ROWS, D), jnp.float32),
        "gain": 1 + 0.1 * jax.random.normal(kn, (D,), jnp.float32),
        "wq": 2 * weights(kq, D, HEADS * HEAD),
        "wk": 2 * weights(kk, D, KV_HEADS * HEAD),
        "wv": 4 * weights(kv, D, KV_HEADS * HEAD),
        "wo": weights(ko, HEADS * HEAD, D),
    }
    return {k: v.astype(jnp.bfloat16) for k, v in drawn.items()}


def normed(x, gain):
    wide = x.astype(jnp.float32)
    scale = lax.rsqrt(jnp.mean(wide * wide, -1, keepdims=True) + 1e-6)
    return (wide * scale * gain.astype(jnp.float32)).astype(jnp.bfloat16)


def turned(t, place, theta):
    half = t.shape[-1] // 2
    angle = place.astype(jnp.float32)[:, None] * theta ** (-jnp.arange(half, dtype=jnp.float32) / half)
    cos, sin = jnp.cos(angle)[:, None], jnp.sin(angle)[:, None]
    a, b = t[..., :half].astype(jnp.float32), t[..., half:].astype(jnp.float32)
    return jnp.concatenate([a * cos - b * sin, b * cos + a * sin], -1).astype(jnp.bfloat16)


def matmul(a, w):
    return jnp.dot(a, w, preferred_element_type=jnp.float32).astype(jnp.bfloat16)


def einsum(form, a, b):
    return jnp.einsum(form, a.astype(jnp.float32), b.astype(jnp.float32))


def attention(q, k, v):
    scores = einsum("tgsd,ugd->gstu", q, k) * q.shape[-1] ** -0.5
    token = jnp.arange(q.shape[0])
    scores = jnp.where(token[:, None] >= token, scores, -jnp.inf)
    weights = jax.nn.softmax(scores, -1).astype(jnp.bfloat16)
    return einsum("gstu,ugd->tgsd", weights, v).astype(jnp.bfloat16)


def reference(x, gain, wq, wk, wv, wo):
    a, place = normed(x, gain), jnp.arange(ROWS)
    q = turned(matmul(a, wq).reshape(ROWS, HEADS, HEAD), place, THETA).reshape(ROWS, KV_HEADS, -1, HEAD)
    k = turned(matmul(a, wk).reshape(ROWS, KV_HEADS, HEAD), place, THETA)
    v = matmul(a, wv).reshape(ROWS, KV_HEADS, HEAD)
    seen = attention(q, k, v).reshape(ROWS, HEADS * HEAD)
    return (x.astype(jnp.float32) + jnp.dot(seen, wo, preferred_element_type=jnp.float32)).astype(jnp.bfloat16)
```

```python
import functools
import math

import jax
import jax.numpy as jnp
from jax import lax
from jax.experimental import pallas as pl
from jax.experimental.pallas import tpu as pltpu
from jax.sharding import PartitionSpec as P

HEAD = 128
THETA = 10000
NEG = -1e30
LOG2E = 1.4426950408889634
E2 = HEAD**-0.5 * LOG2E

OWN = 256
ROWS = 2 * OWN
D = 7168
COLS = D // 2
TILE = 512
TILES = COLS // TILE
JOBS = 3 * TILES
HEADS = TILE // HEAD
HALF = D // 2
OUTS = D // TILE
PARTS = 4
PIECE = OWN // PARTS
BF, F32 = jnp.bfloat16, jnp.float32


def _dot(a, b):
    return jnp.dot(a, b, preferred_element_type=F32)


def _dotg(a, b, ca, cb):
    return lax.dot_general(a, b, (((ca,), (cb,)), ((), ())), preferred_element_type=F32)


def _kernel(x_ref, gain_ref, wq_ref, wk_ref, wv_ref, wo_ref, y_ref, a, wb, qkv, rem, ot, lse_out, lse_in, acc, mine, part, got, tab, xt, yt,
            x_sem, w_sem, as_sem, ar_sem, qs_sem, ls_sem, r_sem, lr_sem, ps_sem, pr_sem, xt_sem, y_sem):
    dp, sp = lax.axis_index("dp"), lax.axis_index("sp")
    chip, core = sp // 2, sp % 2
    peer = (dp, chip * 2 + 1 - core)
    other = (dp, (1 - chip) * 2 + core)
    base = pl.multiple_of(core * OWN, OWN)
    first = chip == 0

    def x_copy(i):
        return pltpu.make_async_copy(x_ref.at[pl.ds(i * PIECE, PIECE), :], a.at[pl.ds(base + i * PIECE, PIECE), :], x_sem.at[i])

    for i in range(PARTS):
        x_copy(i).start()

    def job(j):
        early = jnp.where(first, 2 * TILES, TILES)
        n = jnp.where(j < early, j, j - early)
        pairs = (j < early) == first
        return jnp.where(pairs, 1 + n % 2, 0), jnp.where(pairs, n // 2, n)

    def w_copy(ref, tile, slot, h):
        cols = pl.ds(pl.multiple_of(core * COLS + tile * TILE, TILE), TILE)
        return pltpu.make_async_copy(ref.at[pl.ds(h * HALF, HALF), cols], wb.at[2 * slot + h], w_sem.at[2 * slot + h])

    def w_start(j):
        mat, tile = job(j)
        for m, ref in enumerate((wq_ref, wk_ref, wv_ref)):
            @pl.when(mat == m)
            def _():
                for h in range(2):
                    w_copy(ref, tile, j % 2, h).start()

    def w_wait(j):
        for h in range(2):
            w_copy(wq_ref, 0, j % 2, h).wait()

    def o_copy(u):
        rows = pl.ds(pl.multiple_of(core * COLS, COLS), COLS)
        sub = (u + 2) % 4
        return pltpu.make_async_copy(wo_ref.at[rows, pl.ds(pl.multiple_of(u * TILE, TILE), TILE)], wb.at[sub], w_sem.at[sub])

    w_start(0)

    lse_in[...] = jnp.full(lse_in.shape, NEG, F32)
    lse_out[...] = jnp.zeros(lse_out.shape, F32)

    barrier = pltpu.get_barrier_semaphore()
    for who in (peer, other):
        pl.semaphore_signal(barrier, inc=1, device_id=who, device_id_type=pl.DeviceIdType.MESH)

    place = (chip * ROWS + lax.broadcasted_iota(jnp.int32, (ROWS, HEAD), 0)).astype(F32)
    lane = lax.broadcasted_iota(jnp.int32, (ROWS, HEAD), 1)
    angle = place * jnp.exp2((lane % 64).astype(F32) * (-math.log2(THETA) / 64))
    tab[0, 0] = jnp.cos(angle)
    sin = jnp.sin(angle)
    tab[0, 1] = jnp.where(lane < 64, -sin, sin)
    tab[1, 0] = jnp.ones((ROWS, HEAD), F32)
    tab[1, 1] = jnp.zeros((ROWS, HEAD), F32)

    pl.semaphore_wait(barrier, 2)

    def a_copy(i):
        rows = pl.ds(base + i * PIECE, PIECE)
        return pltpu.make_async_remote_copy(src_ref=a.at[rows, :], dst_ref=a.at[rows, :], send_sem=as_sem.at[i], recv_sem=ar_sem.at[i],
                                            device_id=peer, device_id_type=pl.DeviceIdType.MESH)

    for i in range(PARTS):
        x_copy(i).wait()

        def norm(n, _):
            rows = pl.ds(pl.multiple_of(base + i * PIECE + n * 16, 16), 16)
            wide = a[rows, :].astype(F32)
            scale = lax.rsqrt(jnp.mean(wide * wide, -1, keepdims=True) + 1e-6)
            a[rows, :] = (wide * scale * gain_ref[...].astype(F32)).astype(BF)
            return 0

        lax.fori_loop(0, PIECE // 16, norm, 0)
        a_copy(i).start()

    def epilogue(j):
        mat, tile = job(j)
        kind = jnp.where(mat == 2, 1, 0)
        cos, sin = tab[kind, 0], tab[kind, 1]
        for h in range(HEADS):
            t = acc[:, h * HEAD : (h + 1) * HEAD].astype(BF).astype(F32)
            qkv[mat, tile, :, h * HEAD : (h + 1) * HEAD] = (t * cos + pltpu.roll(t, 64, 1) * sin).astype(BF)

    def q_send(t):
        return pltpu.make_async_remote_copy(src_ref=qkv.at[0, t], dst_ref=rem.at[t], send_sem=qs_sem.at[t], recv_sem=r_sem.at[t],
                                            device_id=other, device_id_type=pl.DeviceIdType.MESH)

    def o_send(t):
        return pltpu.make_async_remote_copy(src_ref=ot.at[t], dst_ref=rem.at[t], send_sem=qs_sem.at[t], recv_sem=r_sem.at[t],
                                            device_id=other, device_id_type=pl.DeviceIdType.MESH)

    def l_send(t):
        return pltpu.make_async_remote_copy(src_ref=lse_out.at[t], dst_ref=lse_in.at[t], send_sem=ls_sem.at[t], recv_sem=lr_sem.at[t],
                                            device_id=other, device_id_type=pl.DeviceIdType.MESH)

    ones = jnp.ones((8, ROWS), BF)

    def strip(q, k, v, mask):
        s = _dotg(k, q, 1, 1)
        if mask:
            n, m = s.shape
            row = lax.broadcasted_iota(jnp.int32, s.shape, 0)
            s = jnp.where(row <= lax.broadcasted_iota(jnp.int32, s.shape, 1) + (n - m), s, 2 * NEG)
        top = s.max(axis=0, keepdims=True)
        p = jnp.exp2((s - top) * E2).astype(BF)
        mix = _dot(jnp.concatenate([v.T, ones[:, : v.shape[0]]], axis=0), p)
        return mix[:HEAD], top * E2, mix[HEAD : HEAD + 1]

    def beyond(t):
        def head(h, _):
            at = pl.ds(pl.multiple_of(h * HEAD, HEAD), HEAD)
            k, v = qkv[1, t, :, at], qkv[2, t, :, at]
            for b in range(2):
                rows = slice(b * OWN, (b + 1) * OWN)
                out, top, total = strip(rem[t, rows, at], k, v, False)
                ot[t, at, rows] = (out * (1 / total)).astype(BF)
                lse_out[t, pl.ds(h, 1), rows] = top + jnp.log2(total)
            return 0

        lax.fori_loop(0, HEADS, head, 0)

    def within(t):
        def head(h, _):
            at = pl.ds(pl.multiple_of(h * HEAD, HEAD), HEAD)
            k, v = qkv[1, t, :, at], qkv[2, t, :, at]
            for b in range(2):
                rows = slice(b * OWN, (b + 1) * OWN)
                out, top, total = strip(qkv[0, t, rows, at], k[: (b + 1) * OWN], v[: (b + 1) * OWN], True)
                far = lse_in[t, pl.ds(h, 1), rows]
                high = jnp.maximum(top, far)
                near, far = jnp.exp2(top - high), jnp.exp2(far - high)
                out = (out * near + rem[t, at, rows].astype(F32) * far) * (1 / (total * near + far))
                qkv[0, t, rows, at] = out.T.astype(BF)
            return 0

        lax.fori_loop(0, HEADS, head, 0)

    w_start(1)
    w_wait(0)

    def part_of_first(n, _):
        @pl.when(n == 1)
        def _():
            for i in range(PARTS):
                a_copy(i).wait_recv()

        rows = pl.ds(pl.multiple_of(((core + n) % 2) * OWN, OWN), OWN)
        acc[rows, :] = _dot(a[rows, :HALF], wb[0]) + _dot(a[rows, HALF:], wb[1])
        return 0

    lax.fori_loop(0, 2, part_of_first, 0)

    def step(j, _):
        w_wait(j)

        @pl.when(j + 1 < JOBS)
        def _():
            w_start(j + 1)

        @pl.when(j + 1 == JOBS)
        def _():
            o_copy(0).start()
            o_copy(1).start()

        epilogue(j - 1)
        slot = 2 * (j % 2)
        acc[...] = _dot(a[:, :HALF], wb[slot]) + _dot(a[:, HALF:], wb[slot + 1])

        @pl.when((chip == 1) & (j - 1 < TILES))
        def _():
            q_send(j - 1).start()

        t = jnp.maximum((j - 6) * 3 + 2, 0) // 7

        @pl.when(first & (j >= 6) & (6 + (7 * t) // 3 == j))
        def _():
            q_send(t).wait_recv()
            beyond(t)
            o_send(t).start()
            l_send(t).start()

        return 0

    lax.fori_loop(1, JOBS, step, 0)
    epilogue(JOBS - 1)
    o_copy(2).start()
    o_copy(3).start()

    def merge(t, _):
        @pl.when(chip == 1)
        def _():
            q_send(t).wait_send()
            o_send(t).wait_recv()
            l_send(t).wait_recv()

        within(t)
        return 0

    lax.fori_loop(0, TILES, merge, 0)

    def x_tile(u):
        return pltpu.make_async_copy(x_ref.at[:, pl.ds(pl.multiple_of(u * TILE, TILE), TILE)], xt.at[u % 3], xt_sem.at[u % 3])

    def y_tile(u):
        return pltpu.make_async_copy(yt.at[u % 2], y_ref.at[:, pl.ds(pl.multiple_of(u * TILE, TILE), TILE)], y_sem.at[u % 2])

    def p_send(u):
        return pltpu.make_async_remote_copy(src_ref=part.at[u % 2], dst_ref=got.at[u], send_sem=ps_sem.at[u % 2], recv_sem=pr_sem.at[u],
                                            device_id=peer, device_id_type=pl.DeviceIdType.MESH)

    def finish(u):
        p_send(u).wait_recv()
        x_tile(u).wait()

        @pl.when(u >= 2)
        def _():
            y_tile(u - 2).wait()

        yt[u % 2] = (xt[u % 3].astype(F32) + (mine[u % 2] + got[u])).astype(BF)
        y_tile(u).start()

    x_tile(0).start()

    def out_step(u, _):
        o_copy(u).wait()

        @pl.when((u >= 1) & (u + 3 < OUTS))
        def _():
            o_copy(u + 3).start()

        @pl.when(u + 1 < OUTS)
        def _():
            x_tile(u + 1).start()

        sub = (u + 2) % 4
        acc[...] = sum(_dot(qkv[0, t], wb[sub, t * TILE : (t + 1) * TILE, :]) for t in range(TILES))

        @pl.when(u >= 2)
        def _():
            p_send(u - 2).wait_send()

        part[u % 2] = acc[pl.ds(OWN - base, OWN), :]
        p_send(u).start()

        @pl.when(u >= 1)
        def _():
            finish(u - 1)

        mine[u % 2] = acc[pl.ds(base, OWN), :]
        return 0

    lax.fori_loop(0, OUTS, out_step, 0)
    finish(OUTS - 1)
    for u in (OUTS - 2, OUTS - 1):
        p_send(u).wait_send()
        y_tile(u).wait()
    for i in range(PARTS):
        a_copy(i).wait_send()

    @pl.when(first)
    def _():
        for t in range(TILES):
            o_send(t).wait_send()
            l_send(t).wait_send()


def solution(mesh):
    def step(x, gain, wq, wk, wv, wo):
        dma = pltpu.SemaphoreType.DMA
        return pl.pallas_call(
            _kernel,
            out_shape=jax.ShapeDtypeStruct((OWN, D), BF),
            in_specs=[pl.BlockSpec(memory_space=pl.ANY), pl.BlockSpec(memory_space=pltpu.VMEM)] + [pl.BlockSpec(memory_space=pl.ANY)] * 4,
            out_specs=pl.BlockSpec(memory_space=pl.ANY),
            scratch_shapes=[
                pltpu.VMEM((ROWS, D), BF),
                pltpu.VMEM((4, HALF, TILE), BF),
                pltpu.VMEM((3, TILES, ROWS, TILE), BF),
                pltpu.VMEM((TILES, ROWS, TILE), BF),
                pltpu.VMEM((TILES, TILE, ROWS), BF),
                pltpu.VMEM((TILES, 8, ROWS), F32),
                pltpu.VMEM((TILES, 8, ROWS), F32),
                pltpu.VMEM((ROWS, TILE), F32),
                pltpu.VMEM((2, OWN, TILE), F32),
                pltpu.VMEM((2, OWN, TILE), F32),
                pltpu.VMEM((OUTS, OWN, TILE), F32),
                pltpu.VMEM((2, 2, ROWS, HEAD), F32),
                pltpu.VMEM((3, OWN, TILE), BF),
                pltpu.VMEM((2, OWN, TILE), BF),
                dma((PARTS,)), dma((4,)), dma((PARTS,)), dma((PARTS,)),
                dma((TILES,)), dma((TILES,)), dma((TILES,)), dma((TILES,)),
                dma((2,)), dma((OUTS,)), dma((3,)), dma((2,)),
            ],
            compiler_params=pltpu.CompilerParams(collective_id=0, has_side_effects=True, vmem_limit_bytes=67043328),
        )(x, gain.reshape(1, D), wq, wk, wv, wo)

    tokens, whole = P(("dp", "sp"), None), P(None, None)
    return jax.shard_map(
        step,
        mesh=mesh,
        in_specs=(tokens, P(None), whole, whole, whole, whole),
        out_specs=tokens,
        check_vma=False,
    )
```

```python
import functools
import math

import jax
import jax.numpy as jnp
from jax import lax
from jax.experimental import pallas as pl
from jax.experimental.pallas import tpu as pltpu
from jax.sharding import PartitionSpec as P

HEAD = 128
THETA = 10000
NEG = -1e30
LOG2E = 1.4426950408889634
E2 = HEAD**-0.5 * LOG2E

OWN = 256
ROWS = 2 * OWN
D = 7168
COLS = D // 2
TILE = 512
TILES = COLS // TILE
JOBS = 3 * TILES
HEADS = TILE // HEAD
HALF = D // 2
OUTS = D // TILE
PARTS = 4
PIECE = OWN // PARTS
BF, F32 = jnp.bfloat16, jnp.float32


def _dot(a, b):
    return jnp.dot(a, b, preferred_element_type=F32)


def _dotg(a, b, ca, cb):
    return lax.dot_general(a, b, (((ca,), (cb,)), ((), ())), preferred_element_type=F32)


def _kernel(x_ref, gain_ref, wq_ref, wk_ref, wv_ref, wo_ref, y_ref, a, wb, qkv, rem, ot, lse_out, lse_in, acc, mine, part, got, tab, xt, yt,
            x_sem, w_sem, as_sem, ar_sem, qs_sem, ls_sem, r_sem, lr_sem, ps_sem, pr_sem, xt_sem, y_sem):
    dp, sp = lax.axis_index("dp"), lax.axis_index("sp")
    chip, core = sp // 2, sp % 2
    peer = (dp, chip * 2 + 1 - core)
    other = (dp, (1 - chip) * 2 + core)
    base = pl.multiple_of(core * OWN, OWN)
    first = chip == 0

    def x_copy(i):
        return pltpu.make_async_copy(x_ref.at[pl.ds(i * PIECE, PIECE), :], a.at[pl.ds(base + i * PIECE, PIECE), :], x_sem.at[i])

    for i in range(PARTS):
        x_copy(i).start()

    lse_in[...] = jnp.full(lse_in.shape, NEG, F32)
    lse_out[...] = jnp.zeros(lse_out.shape, F32)

    barrier = pltpu.get_barrier_semaphore()
    for who in (peer, other):
        pl.semaphore_signal(barrier, inc=1, device_id=who, device_id_type=pl.DeviceIdType.MESH)

    def job(j):
        early = jnp.where(first, 2 * TILES, TILES)
        n = jnp.where(j < early, j, j - early)
        pairs = (j < early) == first
        return jnp.where(pairs, 1 + n % 2, 0), jnp.where(pairs, n // 2, n)

    def w_copy(ref, tile, slot, h):
        cols = pl.ds(pl.multiple_of(core * COLS + tile * TILE, TILE), TILE)
        return pltpu.make_async_copy(ref.at[pl.ds(h * HALF, HALF), cols], wb.at[2 * slot + h], w_sem.at[2 * slot + h])

    def w_start(j):
        mat, tile = job(j)
        for m, ref in enumerate((wq_ref, wk_ref, wv_ref)):
            @pl.when(mat == m)
            def _():
                for h in range(2):
                    w_copy(ref, tile, j % 2, h).start()

    def w_wait(j):
        for h in range(2):
            w_copy(wq_ref, 0, j % 2, h).wait()

    def o_copy(u):
        rows = pl.ds(pl.multiple_of(core * COLS, COLS), COLS)
        sub = (u + 2) % 4
        return pltpu.make_async_copy(wo_ref.at[rows, pl.ds(pl.multiple_of(u * TILE, TILE), TILE)], wb.at[sub], w_sem.at[sub])

    w_start(0)

    w_start(1)

    pl.semaphore_wait(barrier, 2)

    def a_copy(i):
        return pltpu.make_async_remote_copy(src_ref=x_ref.at[pl.ds(i * PIECE, PIECE), :], dst_ref=a.at[pl.ds(base + i * PIECE, PIECE), :],
                                            send_sem=as_sem.at[i], recv_sem=ar_sem.at[i], device_id=peer, device_id_type=pl.DeviceIdType.MESH)

    for i in range(PARTS):
        a_copy(i).start()

    place = (chip * ROWS + lax.broadcasted_iota(jnp.int32, (ROWS, HEAD), 0)).astype(F32)
    lane = lax.broadcasted_iota(jnp.int32, (ROWS, HEAD), 1)
    angle = place * jnp.exp2((lane % 64).astype(F32) * (-math.log2(THETA) / 64))
    tab[0, 0] = jnp.cos(angle)
    sin = jnp.sin(angle)
    tab[0, 1] = jnp.where(lane < 64, -sin, sin)
    tab[1, 0] = jnp.ones((ROWS, HEAD), F32)
    tab[1, 1] = jnp.zeros((ROWS, HEAD), F32)

    def norm(at, i):
        def few(n, _):
            rows = pl.ds(pl.multiple_of(at + i * PIECE + n * 16, 16), 16)
            wide = a[rows, :].astype(F32)
            scale = lax.rsqrt(jnp.mean(wide * wide, -1, keepdims=True) + 1e-6)
            a[rows, :] = (wide * scale * gain_ref[...].astype(F32)).astype(BF)
            return 0

        lax.fori_loop(0, PIECE // 16, few, 0)

    for i in range(PARTS):
        x_copy(i).wait()
        norm(base, i)

    def epilogue(j):
        mat, tile = job(j)
        kind = jnp.where(mat == 2, 1, 0)
        cos, sin = tab[kind, 0], tab[kind, 1]
        for h in range(HEADS):
            t = acc[0, :, h * HEAD : (h + 1) * HEAD].astype(BF).astype(F32)
            qkv[mat, tile, :, h * HEAD : (h + 1) * HEAD] = (t * cos + pltpu.roll(t, 64, 1) * sin).astype(BF)

    def q_send(t):
        return pltpu.make_async_remote_copy(src_ref=qkv.at[0, t], dst_ref=rem.at[t], send_sem=qs_sem.at[t], recv_sem=r_sem.at[t],
                                            device_id=other, device_id_type=pl.DeviceIdType.MESH)

    def o_send(t):
        return pltpu.make_async_remote_copy(src_ref=ot.at[t], dst_ref=rem.at[t], send_sem=qs_sem.at[t], recv_sem=r_sem.at[t],
                                            device_id=other, device_id_type=pl.DeviceIdType.MESH)

    def l_send(t):
        return pltpu.make_async_remote_copy(src_ref=lse_out.at[t], dst_ref=lse_in.at[t], send_sem=ls_sem.at[t], recv_sem=lr_sem.at[t],
                                            device_id=other, device_id_type=pl.DeviceIdType.MESH)

    ones = jnp.ones((8, ROWS), BF)

    def strips(items, mask):
        weights, outs = [], []
        scores = [_dotg(k, q, 1, 1) for q, k, _ in items]
        for s in scores:
            if mask:
                n, m = s.shape
                row = lax.broadcasted_iota(jnp.int32, s.shape, 0)
                s = jnp.where(row <= lax.broadcasted_iota(jnp.int32, s.shape, 1) + (n - m), s, 2 * NEG)
            top = s.max(axis=0, keepdims=True)
            weights.append((jnp.exp2((s - top) * E2).astype(BF), top * E2))
        for (_, _, v), (p, top) in zip(items, weights):
            mix = _dot(jnp.concatenate([v.T, ones[:, : v.shape[0]]], axis=0), p)
            outs.append((mix[:HEAD], top, mix[HEAD : HEAD + 1]))
        return outs

    places = [(h, slice(h * HEAD, (h + 1) * HEAD), slice(b * OWN, (b + 1) * OWN)) for h in range(HEADS) for b in range(2)]

    def beyond(t):
        items = [(rem[t, rows, at], qkv[1, t, :, at], qkv[2, t, :, at]) for _, at, rows in places]
        for (h, at, rows), (out, top, total) in zip(places, strips(items, False)):
            ot[t, at, rows] = (out * (1 / total)).astype(BF)
            lse_out[t, h : h + 1, rows] = top + jnp.log2(total)

    def within(t):
        items = [(qkv[0, t, rows, at], qkv[1, t, : rows.stop, at], qkv[2, t, : rows.stop, at]) for _, at, rows in places]
        for (h, at, rows), (out, top, total) in zip(places, strips(items, True)):
            far = lse_in[t, h : h + 1, rows]
            high = jnp.maximum(top, far)
            near, far = jnp.exp2(top - high), jnp.exp2(far - high)
            out = (out * near + rem[t, at, rows].astype(F32) * far) * (1 / (total * near + far))
            qkv[0, t, rows, at] = out.T.astype(BF)

    def half_job(n, _):
        j = n % 2

        @pl.when(n < 2)
        def _():
            w_wait(j)

        @pl.when(n == 2)
        def _():
            for i in range(PARTS):
                a_copy(i).wait_recv()
                norm(OWN - base, i)

        rows = pl.ds(pl.multiple_of(((core + n // 2) % 2) * OWN, OWN), OWN)
        acc[j, rows, :] = _dot(a[rows, :HALF], wb[2 * j]) + _dot(a[rows, HALF:], wb[2 * j + 1])

        @pl.when(n == 2)
        def _():
            w_start(2)
            epilogue(0)

            @pl.when(chip == 1)
            def _():
                q_send(0).start()

        return 0

    lax.fori_loop(0, 4, half_job, 0)
    acc[0] = acc[1]

    def step(j, _):
        w_wait(j)

        @pl.when(j + 1 < JOBS)
        def _():
            w_start(j + 1)

        @pl.when(j + 1 == JOBS)
        def _():
            o_copy(0).start()
            o_copy(1).start()

        epilogue(j - 1)
        slot = 2 * (j % 2)
        acc[0] = _dot(a[:, :HALF], wb[slot]) + _dot(a[:, HALF:], wb[slot + 1])

        @pl.when((chip == 1) & (j - 1 < TILES))
        def _():
            q_send(j - 1).start()

        t = jnp.maximum(2 * j - 8, 0) // 5

        @pl.when(first & (j >= 4) & ((9 + 5 * t) // 2 == j))
        def _():
            q_send(t).wait_recv()
            beyond(t)
            o_send(t).start()
            l_send(t).start()

        return 0

    lax.fori_loop(2, JOBS, step, 0)
    epilogue(JOBS - 1)
    o_copy(2).start()
    o_copy(3).start()

    def merge(t, _):
        @pl.when(chip == 1)
        def _():
            q_send(t).wait_send()
            o_send(t).wait_recv()
            l_send(t).wait_recv()

        within(t)
        return 0

    lax.fori_loop(0, TILES, merge, 0)

    def x_tile(u):
        return pltpu.make_async_copy(x_ref.at[:, pl.ds(pl.multiple_of(u * TILE, TILE), TILE)], xt.at[u % 3], xt_sem.at[u % 3])

    def y_tile(u):
        return pltpu.make_async_copy(yt.at[u % 2], y_ref.at[:, pl.ds(pl.multiple_of(u * TILE, TILE), TILE)], y_sem.at[u % 2])

    def p_send(u):
        return pltpu.make_async_remote_copy(src_ref=part.at[u % 2], dst_ref=got.at[u], send_sem=ps_sem.at[u % 2], recv_sem=pr_sem.at[u],
                                            device_id=peer, device_id_type=pl.DeviceIdType.MESH)

    def finish(u):
        p_send(u).wait_recv()
        x_tile(u).wait()

        @pl.when(u >= 2)
        def _():
            y_tile(u - 2).wait()

        yt[u % 2] = (xt[u % 3].astype(F32) + (mine[u % 2] + got[u])).astype(BF)
        y_tile(u).start()

    x_tile(0).start()

    def out_step(u, _):
        o_copy(u).wait()

        @pl.when((u >= 1) & (u + 3 < OUTS))
        def _():
            o_copy(u + 3).start()

        @pl.when(u + 1 < OUTS)
        def _():
            x_tile(u + 1).start()

        sub = (u + 2) % 4
        acc[0] = sum(_dot(qkv[0, t], wb[sub, t * TILE : (t + 1) * TILE, :]) for t in range(TILES))

        @pl.when(u >= 2)
        def _():
            p_send(u - 2).wait_send()

        part[u % 2] = acc[0, pl.ds(OWN - base, OWN), :]
        p_send(u).start()

        @pl.when(u >= 1)
        def _():
            finish(u - 1)

        mine[u % 2] = acc[0, pl.ds(base, OWN), :]
        return 0

    lax.fori_loop(0, OUTS, out_step, 0)
    finish(OUTS - 1)
    for u in (OUTS - 2, OUTS - 1):
        p_send(u).wait_send()
        y_tile(u).wait()
    for i in range(PARTS):
        a_copy(i).wait_send()

    @pl.when(first)
    def _():
        for t in range(TILES):
            o_send(t).wait_send()
            l_send(t).wait_send()


def solution(mesh):
    def step(x, gain, wq, wk, wv, wo):
        dma = pltpu.SemaphoreType.DMA
        return pl.pallas_call(
            _kernel,
            out_shape=jax.ShapeDtypeStruct((OWN, D), BF),
            in_specs=[pl.BlockSpec(memory_space=pl.ANY), pl.BlockSpec(memory_space=pltpu.VMEM)] + [pl.BlockSpec(memory_space=pl.ANY)] * 4,
            out_specs=pl.BlockSpec(memory_space=pl.ANY),
            scratch_shapes=[
                pltpu.VMEM((ROWS, D), BF),
                pltpu.VMEM((4, HALF, TILE), BF),
                pltpu.VMEM((3, TILES, ROWS, TILE), BF),
                pltpu.VMEM((TILES, ROWS, TILE), BF),
                pltpu.VMEM((TILES, TILE, ROWS), BF),
                pltpu.VMEM((TILES, 8, ROWS), F32),
                pltpu.VMEM((TILES, 8, ROWS), F32),
                pltpu.VMEM((2, ROWS, TILE), F32),
                pltpu.VMEM((2, OWN, TILE), F32),
                pltpu.VMEM((2, OWN, TILE), F32),
                pltpu.VMEM((OUTS, OWN, TILE), F32),
                pltpu.VMEM((2, 2, ROWS, HEAD), F32),
                pltpu.VMEM((3, OWN, TILE), BF),
                pltpu.VMEM((2, OWN, TILE), BF),
                dma((PARTS,)), dma((4,)), dma((PARTS,)), dma((PARTS,)),
                dma((TILES,)), dma((TILES,)), dma((TILES,)), dma((TILES,)),
                dma((2,)), dma((OUTS,)), dma((3,)), dma((2,)),
            ],
            compiler_params=pltpu.CompilerParams(collective_id=0, has_side_effects=True, vmem_limit_bytes=67043328),
        )(x, gain, wq, wk, wv, wo)

    tokens, whole = P(("dp", "sp"), None), P(None, None)
    return jax.shard_map(
        step,
        mesh=mesh,
        in_specs=(tokens, P(None), whole, whole, whole, whole),
        out_specs=tokens,
        check_vma=False,
    )
```

```python
import functools
import math

import jax
import jax.numpy as jnp
from jax import lax
from jax.experimental import pallas as pl
from jax.experimental.pallas import tpu as pltpu
from jax.sharding import PartitionSpec as P

HEAD = 128
THETA = 10000
NEG = -1e30
LOG2E = 1.4426950408889634
E2 = HEAD**-0.5 * LOG2E

OWN = 256
ROWS = 2 * OWN
D = 7168
COLS = D // 2
TILE = 512
TILES = COLS // TILE
JOBS = 3 * TILES
HEADS = TILE // HEAD
HALF = D // 2
OUTS = D // TILE
PARTS = 4
PIECE = OWN // PARTS
BF, F32 = jnp.bfloat16, jnp.float32


def _dot(a, b):
    return jnp.dot(a, b, preferred_element_type=F32)


def _dotg(a, b, ca, cb):
    return lax.dot_general(a, b, (((ca,), (cb,)), ((), ())), preferred_element_type=F32)


def _kernel(x_ref, gain_ref, wq_ref, wk_ref, wv_ref, wo_ref, y_ref, a, wb, qkv, rem, ot, lse_out, lse_in, acc, got, tab, xt, yt,
            x_sem, w_sem, as_sem, ar_sem, qs_sem, ls_sem, r_sem, lr_sem, ps_sem, pr_sem, xt_sem, y_sem):
    dp, sp = lax.axis_index("dp"), lax.axis_index("sp")
    chip, core = sp // 2, sp % 2
    peer = (dp, chip * 2 + 1 - core)
    other = (dp, (1 - chip) * 2 + core)
    base = pl.multiple_of(core * OWN, OWN)
    first = chip == 0

    def x_copy(i):
        return pltpu.make_async_copy(x_ref.at[pl.ds(i * PIECE, PIECE), :], a.at[pl.ds(base + i * PIECE, PIECE), :], x_sem.at[i])

    for i in range(PARTS):
        x_copy(i).start()

    lse_in[...] = jnp.full(lse_in.shape, NEG, F32)
    lse_out[...] = jnp.zeros(lse_out.shape, F32)

    barrier = pltpu.get_barrier_semaphore()
    for who in (peer, other):
        pl.semaphore_signal(barrier, inc=1, device_id=who, device_id_type=pl.DeviceIdType.MESH)

    def job(j):
        early = jnp.where(first, 2 * TILES, TILES)
        n = jnp.where(j < early, j, j - early)
        pairs = (j < early) == first
        return jnp.where(pairs, 1 + n % 2, 0), jnp.where(pairs, n // 2, n)

    def w_copy(ref, tile, slot, h):
        cols = pl.ds(pl.multiple_of(core * COLS + tile * TILE, TILE), TILE)
        return pltpu.make_async_copy(ref.at[pl.ds(h * HALF, HALF), cols], wb.at[2 * slot + h], w_sem.at[2 * slot + h])

    def w_start(j):
        mat, tile = job(j)
        for m, ref in enumerate((wq_ref, wk_ref, wv_ref)):
            @pl.when(mat == m)
            def _():
                for h in range(2):
                    w_copy(ref, tile, j % 2, h).start()

    def w_wait(j):
        for h in range(2):
            w_copy(wq_ref, 0, j % 2, h).wait()

    def o_copy(u):
        rows = pl.ds(pl.multiple_of(core * COLS, COLS), COLS)
        sub = (u + 2) % 4
        return pltpu.make_async_copy(wo_ref.at[rows, pl.ds(pl.multiple_of(u * TILE, TILE), TILE)], wb.at[sub], w_sem.at[sub])

    w_start(0)

    place = (chip * ROWS + lax.broadcasted_iota(jnp.int32, (ROWS, HEAD), 0)).astype(F32)
    lane = lax.broadcasted_iota(jnp.int32, (ROWS, HEAD), 1)
    angle = place * jnp.exp2((lane % 64).astype(F32) * (-math.log2(THETA) / 64))
    tab[0, 0] = jnp.cos(angle)
    sin = jnp.sin(angle)
    tab[0, 1] = jnp.where(lane < 64, -sin, sin)
    tab[1, 0] = jnp.ones((ROWS, HEAD), F32)
    tab[1, 1] = jnp.zeros((ROWS, HEAD), F32)

    pl.semaphore_wait(barrier, 2)

    def a_copy(i):
        rows = pl.ds(base + i * PIECE, PIECE)
        return pltpu.make_async_remote_copy(src_ref=a.at[rows, :], dst_ref=a.at[rows, :], send_sem=as_sem.at[i], recv_sem=ar_sem.at[i],
                                            device_id=peer, device_id_type=pl.DeviceIdType.MESH)

    gain = gain_ref[...].astype(F32)
    for i in range(PARTS):
        x_copy(i).wait()
        if i == PARTS - 1:
            w_start(1)
        rows = pl.ds(base + i * PIECE, PIECE)
        wide = a[rows, :].astype(F32)
        scale = lax.rsqrt(jnp.mean(wide * wide, -1, keepdims=True) + 1e-6)
        a[rows, :] = (a[rows, :].astype(F32) * scale * gain).astype(BF)
        a_copy(i).start()

    def epilogue(j):
        mat, tile = job(j)
        kind = jnp.where(mat == 2, 1, 0)
        cos, sin = tab[kind, 0], tab[kind, 1]
        for h in range(HEADS):
            t = acc[0, :, h * HEAD : (h + 1) * HEAD].astype(BF).astype(F32)
            qkv[mat, tile, :, h * HEAD : (h + 1) * HEAD] = (t * cos + pltpu.roll(t, 64, 1) * sin).astype(BF)

    def q_send(t):
        return pltpu.make_async_remote_copy(src_ref=qkv.at[0, t], dst_ref=rem.at[t], send_sem=qs_sem.at[t], recv_sem=r_sem.at[t],
                                            device_id=other, device_id_type=pl.DeviceIdType.MESH)

    def o_send(t):
        return pltpu.make_async_remote_copy(src_ref=ot.at[t], dst_ref=rem.at[t], send_sem=qs_sem.at[t], recv_sem=r_sem.at[t],
                                            device_id=other, device_id_type=pl.DeviceIdType.MESH)

    def l_send(t):
        return pltpu.make_async_remote_copy(src_ref=lse_out.at[t], dst_ref=lse_in.at[t], send_sem=ls_sem.at[t], recv_sem=lr_sem.at[t],
                                            device_id=other, device_id_type=pl.DeviceIdType.MESH)

    ones = jnp.ones((8, ROWS), BF)

    def strips(items, mask):
        weights, outs = [], []
        scores = [_dotg(k, q, 1, 1) for q, k, _ in items]
        for s in scores:
            if mask:
                n, m = s.shape
                row = lax.broadcasted_iota(jnp.int32, s.shape, 0)
                s = jnp.where(row <= lax.broadcasted_iota(jnp.int32, s.shape, 1) + (n - m), s, 2 * NEG)
            top = s.max(axis=0, keepdims=True)
            weights.append((jnp.exp2((s - top) * E2).astype(BF), top * E2))
        for (_, _, v), (p, top) in zip(items, weights):
            mix = _dot(jnp.concatenate([v.T, ones[:, : v.shape[0]]], axis=0), p)
            outs.append((mix[:HEAD], top, mix[HEAD : HEAD + 1]))
        return outs

    places = [(h, slice(h * HEAD, (h + 1) * HEAD), slice(b * OWN, (b + 1) * OWN)) for h in range(HEADS) for b in range(2)]

    def beyond(t):
        items = [(rem[t, rows, at], qkv[1, t, :, at], qkv[2, t, :, at]) for _, at, rows in places]
        for (h, at, rows), (out, top, total) in zip(places, strips(items, False)):
            ot[t, at, rows] = (out * (1 / total)).astype(BF)
            lse_out[t, h : h + 1, rows] = top + jnp.log2(total)

    def within(t):
        items = [(qkv[0, t, rows, at], qkv[1, t, : rows.stop, at], qkv[2, t, : rows.stop, at]) for _, at, rows in places]
        for (h, at, rows), (out, top, total) in zip(places, strips(items, True)):
            far = lse_in[t, h : h + 1, rows]
            high = jnp.maximum(top, far)
            near, far = jnp.exp2(top - high), jnp.exp2(far - high)
            out = (out * near + rem[t, at, rows].astype(F32) * far) * (1 / (total * near + far))
            qkv[0, t, rows, at] = out.T.astype(BF)

    def half_job(n, _):
        j = n % 2

        @pl.when(n < 2)
        def _():
            w_wait(j)

        @pl.when(n == 2)
        def _():
            for i in range(PARTS):
                a_copy(i).wait_recv()

        rows = pl.ds(pl.multiple_of(((core + n // 2) % 2) * OWN, OWN), OWN)
        acc[j, rows, :] = _dot(a[rows, :HALF], wb[2 * j]) + _dot(a[rows, HALF:], wb[2 * j + 1])

        @pl.when(n == 2)
        def _():
            w_start(2)
            epilogue(0)

            @pl.when(chip == 1)
            def _():
                q_send(0).start()

        return 0

    lax.fori_loop(0, 4, half_job, 0)
    acc[0] = acc[1]

    def step(j, _):
        w_wait(j)

        @pl.when(j + 1 < JOBS)
        def _():
            w_start(j + 1)

        @pl.when(j + 1 == JOBS)
        def _():
            o_copy(0).start()
            o_copy(1).start()

        epilogue(j - 1)
        slot = 2 * (j % 2)
        acc[0] = _dot(a[:, :HALF], wb[slot]) + _dot(a[:, HALF:], wb[slot + 1])

        @pl.when((chip == 1) & (j - 1 < TILES))
        def _():
            q_send(j - 1).start()

        t = jnp.maximum(2 * j - 8, 0) // 5

        @pl.when(first & (j >= 4) & ((9 + 5 * t) // 2 == j))
        def _():
            q_send(t).wait_recv()
            beyond(t)
            o_send(t).start()
            l_send(t).start()

        return 0

    lax.fori_loop(2, JOBS, step, 0)
    epilogue(JOBS - 1)
    o_copy(2).start()
    o_copy(3).start()

    def merge(t, _):
        @pl.when(chip == 1)
        def _():
            q_send(t).wait_send()
            o_send(t).wait_recv()
            l_send(t).wait_recv()

        within(t)
        return 0

    lax.fori_loop(0, TILES, merge, 0)

    def x_tile(u):
        return pltpu.make_async_copy(x_ref.at[:, pl.ds(pl.multiple_of(u * TILE, TILE), TILE)], xt.at[u % 3], xt_sem.at[u % 3])

    def y_tile(u):
        return pltpu.make_async_copy(yt.at[u % 2], y_ref.at[:, pl.ds(pl.multiple_of(u * TILE, TILE), TILE)], y_sem.at[u % 2])

    def p_send(u):
        return pltpu.make_async_remote_copy(src_ref=acc.at[u % 3, pl.ds(OWN - base, OWN), :], dst_ref=got.at[u], send_sem=ps_sem.at[u % 3],
                                            recv_sem=pr_sem.at[u], device_id=peer, device_id_type=pl.DeviceIdType.MESH)

    def ready(u):
        o_copy(u).wait()
        x_tile(u).start()

        @pl.when((u >= 1) & (u + 3 < OUTS))
        def _():
            o_copy(u + 3).start()

    def project(u):
        sub = (u + 2) % 4
        acc[u % 3] = sum(_dot(qkv[0, t], wb[sub, t * TILE : (t + 1) * TILE, :]) for t in range(TILES))

    def finish(u):
        yt[u % 2] = (xt[u % 3].astype(F32) + (acc[u % 3, pl.ds(base, OWN), :] + got[u])).astype(BF)

    def opening(u, _):
        ready(u)
        project(u)
        p_send(u).start()
        return 0

    lax.fori_loop(0, 2, opening, 0)

    def out_step(u, _):
        ready(u)

        @pl.when(u >= 3)
        def _():
            p_send(u - 3).wait_send()

        @pl.when(u >= 4)
        def _():
            y_tile(u - 4).wait()

        p_send(u - 2).wait_recv()
        x_tile(u - 2).wait()
        finish(u - 2)
        project(u)
        p_send(u).start()
        y_tile(u - 2).start()
        return 0

    lax.fori_loop(2, OUTS, out_step, 0)
    for u in (OUTS - 2, OUTS - 1):
        y_tile(u - 2).wait()
        p_send(u).wait_recv()
        x_tile(u).wait()
        finish(u)
        y_tile(u).start()
    for u in range(OUTS - 3, OUTS):
        p_send(u).wait_send()
    for u in (OUTS - 2, OUTS - 1):
        y_tile(u).wait()
    for i in range(PARTS):
        a_copy(i).wait_send()

    @pl.when(first)
    def _():
        for t in range(TILES):
            o_send(t).wait_send()
            l_send(t).wait_send()


def solution(mesh):
    def step(x, gain, wq, wk, wv, wo):
        dma = pltpu.SemaphoreType.DMA
        return pl.pallas_call(
            _kernel,
            out_shape=jax.ShapeDtypeStruct((OWN, D), BF),
            in_specs=[pl.BlockSpec(memory_space=pl.ANY), pl.BlockSpec(memory_space=pltpu.VMEM)] + [pl.BlockSpec(memory_space=pl.ANY)] * 4,
            out_specs=pl.BlockSpec(memory_space=pl.ANY),
            scratch_shapes=[
                pltpu.VMEM((ROWS, D), BF),
                pltpu.VMEM((4, HALF, TILE), BF),
                pltpu.VMEM((3, TILES, ROWS, TILE), BF),
                pltpu.VMEM((TILES, ROWS, TILE), BF),
                pltpu.VMEM((TILES, TILE, ROWS), BF),
                pltpu.VMEM((TILES, 8, ROWS), F32),
                pltpu.VMEM((TILES, 8, ROWS), F32),
                pltpu.VMEM((3, ROWS, TILE), F32),
                pltpu.VMEM((OUTS, OWN, TILE), F32),
                pltpu.VMEM((2, 2, ROWS, HEAD), F32),
                pltpu.VMEM((3, OWN, TILE), BF),
                pltpu.VMEM((2, OWN, TILE), BF),
                dma((PARTS,)), dma((4,)), dma((PARTS,)), dma((PARTS,)),
                dma((TILES,)), dma((TILES,)), dma((TILES,)), dma((TILES,)),
                dma((3,)), dma((OUTS,)), dma((3,)), dma((2,)),
            ],
            compiler_params=pltpu.CompilerParams(collective_id=0, has_side_effects=True, vmem_limit_bytes=67043328),
        )(x, gain, wq, wk, wv, wo)

    tokens, whole = P(("dp", "sp"), None), P(None, None)
    return jax.shard_map(
        step,
        mesh=mesh,
        in_specs=(tokens, P(None), whole, whole, whole, whole),
        out_specs=tokens,
        check_vma=False,
    )
```

```python
import functools
import math

import jax
import jax.numpy as jnp
from jax import lax
from jax.experimental import pallas as pl
from jax.experimental.pallas import tpu as pltpu
from jax.sharding import PartitionSpec as P

HEAD = 128
THETA = 10000
NEG = -1e30
LOG2E = 1.4426950408889634
E2 = HEAD**-0.5 * LOG2E

OWN = 256
ROWS = 2 * OWN
D = 7168
COLS = D // 2
TILE = 512
TILES = COLS // TILE
JOBS = 3 * TILES
HEADS = TILE // HEAD
HALF = D // 2
OUTS = D // TILE
PARTS = 4
PIECE = OWN // PARTS
BF, F32 = jnp.bfloat16, jnp.float32
Q, K, V, REM, OT = (n * TILES for n in range(5))
LAST = TILES - 1


def _dot(a, b):
    return jnp.dot(a, b, preferred_element_type=F32)


def _dotg(a, b, ca, cb):
    return lax.dot_general(a, b, (((ca,), (cb,)), ((), ())), preferred_element_type=F32)


def _kernel(x_ref, gain_ref, wq_ref, wk_ref, wv_ref, wo_ref, y_ref, a, wb, buf, lse, acc, got, tab, xt, yt,
            x_sem, w_sem, as_sem, ar_sem, qs_sem, ls_sem, r_sem, lr_sem, ps_sem, pr_sem, xt_sem, y_sem):
    dp, sp = lax.axis_index("dp"), lax.axis_index("sp")
    chip, core = sp // 2, sp % 2
    peer = (dp, chip * 2 + 1 - core)
    other = (dp, (1 - chip) * 2 + core)
    base = pl.multiple_of(core * OWN, OWN)
    first = chip == 0

    def x_copy(i):
        return pltpu.make_async_copy(x_ref.at[pl.ds(i * PIECE, PIECE), :], a.at[pl.ds(base + i * PIECE, PIECE), :], x_sem.at[i])

    for i in range(PARTS):
        x_copy(i).start()

    lse[0] = jnp.full(lse.shape[1:], NEG, F32)
    lse[1] = jnp.zeros(lse.shape[1:], F32)
    buf[REM + LAST] = jnp.zeros((ROWS, TILE), BF)

    barrier = pltpu.get_barrier_semaphore()
    for who in (peer, other):
        pl.semaphore_signal(barrier, inc=1, device_id=who, device_id_type=pl.DeviceIdType.MESH)

    def job(j):
        early = jnp.where(first, 2 * TILES, TILES)
        n = jnp.where(j < early, j, j - early)
        pairs = (j < early) == first
        return jnp.where(pairs, 1 + n % 2, 0), jnp.where(pairs, (n // 2 + LAST) % TILES, n)

    def w_copy(ref, tile, slot, h):
        cols = pl.ds(pl.multiple_of(core * COLS + tile * TILE, TILE), TILE)
        return pltpu.make_async_copy(ref.at[pl.ds(h * HALF, HALF), cols], wb.at[2 * slot + h], w_sem.at[2 * slot + h])

    def w_start(j):
        mat, tile = job(j)
        for m, ref in enumerate((wq_ref, wk_ref, wv_ref)):
            @pl.when(mat == m)
            def _():
                for h in range(2):
                    w_copy(ref, tile, j % 2, h).start()

    def w_wait(j):
        for h in range(2):
            w_copy(wq_ref, 0, j % 2, h).wait()

    def o_copy(u):
        rows = pl.ds(pl.multiple_of(core * COLS, COLS), COLS)
        sub = (u + 2) % 4
        return pltpu.make_async_copy(wo_ref.at[rows, pl.ds(pl.multiple_of(u * TILE, TILE), TILE)], wb.at[sub], w_sem.at[sub])

    w_start(0)

    place = (chip * ROWS + lax.broadcasted_iota(jnp.int32, (ROWS, HEAD), 0)).astype(F32)
    lane = lax.broadcasted_iota(jnp.int32, (ROWS, HEAD), 1)
    angle = place * jnp.exp2((lane % 64).astype(F32) * (-math.log2(THETA) / 64))
    tab[0, 0] = jnp.cos(angle)
    sin = jnp.sin(angle)
    tab[0, 1] = jnp.where(lane < 64, -sin, sin)
    tab[1, 0] = jnp.ones((ROWS, HEAD), F32)
    tab[1, 1] = jnp.zeros((ROWS, HEAD), F32)

    def a_copy(i):
        rows = pl.ds(base + i * PIECE, PIECE)
        return pltpu.make_async_remote_copy(src_ref=a.at[rows, :], dst_ref=a.at[rows, :], send_sem=as_sem.at[i], recv_sem=ar_sem.at[i],
                                            device_id=peer, device_id_type=pl.DeviceIdType.MESH)

    gain = gain_ref[...].astype(F32)
    for i in range(PARTS):
        x_copy(i).wait()
        if i == PARTS - 1:
            w_start(1)
        rows = pl.ds(base + i * PIECE, PIECE)
        wide = a[rows, :].astype(F32)
        scale = lax.rsqrt(jnp.mean(wide * wide, -1, keepdims=True) + 1e-6)
        a[rows, :] = (a[rows, :].astype(F32) * scale * gain).astype(BF)
        if i == 1:
            pl.semaphore_wait(barrier, 2)
            a_copy(0).start()
        if i:
            a_copy(i).start()

    def epilogue(j):
        mat, tile = job(j)
        kind = jnp.where(mat == 2, 1, 0)
        cos, sin = tab[kind, 0], tab[kind, 1]
        for h in range(HEADS):
            t = acc[0, :, h * HEAD : (h + 1) * HEAD].astype(BF).astype(F32)
            buf[mat * TILES + tile, :, h * HEAD : (h + 1) * HEAD] = (t * cos + pltpu.roll(t, 64, 1) * sin).astype(BF)

    def move(src, dst, n):
        return pltpu.make_async_remote_copy(src_ref=buf.at[src], dst_ref=buf.at[dst], send_sem=qs_sem.at[n], recv_sem=r_sem.at[n],
                                            device_id=other, device_id_type=pl.DeviceIdType.MESH)

    def q_send(t):
        return move(Q + t, REM + t, t)

    def o_send(t):
        return move(OT + t, REM + t, t)

    k_send, v_send = move(K + LAST, OT, LAST), move(V + LAST, OT + 1, TILES)

    def l_send(t):
        return pltpu.make_async_remote_copy(src_ref=lse.at[1, t], dst_ref=lse.at[0, t], send_sem=ls_sem.at[t], recv_sem=lr_sem.at[t],
                                            device_id=other, device_id_type=pl.DeviceIdType.MESH)

    ones = jnp.ones((8, ROWS), BF)

    def strips(items, mask):
        weights, outs = [], []
        scores = [_dotg(k, q, 1, 1) for q, k, _ in items]
        for s in scores:
            if mask:
                n, m = s.shape
                row = lax.broadcasted_iota(jnp.int32, s.shape, 0)
                s = jnp.where(row <= lax.broadcasted_iota(jnp.int32, s.shape, 1) + (n - m), s, 2 * NEG)
            top = s.max(axis=0, keepdims=True)
            weights.append((jnp.exp2((s - top) * E2).astype(BF), top * E2))
        for (_, _, v), (p, top) in zip(items, weights):
            mix = _dot(jnp.concatenate([v.T, ones[:, : v.shape[0]]], axis=0), p)
            outs.append((mix[:HEAD], top, mix[HEAD : HEAD + 1]))
        return outs

    places = [(h, slice(h * HEAD, (h + 1) * HEAD), slice(b * OWN, (b + 1) * OWN)) for h in range(HEADS) for b in range(2)]

    def beyond(t):
        q, k, v = jnp.where(first, REM, Q) + t, jnp.where(first, K + t, OT), jnp.where(first, V + t, OT + 1)
        to, side = jnp.where(first, OT, REM) + t, jnp.where(first, 1, 0)
        items = [(buf[q, rows, at], buf[k, :, at], buf[v, :, at]) for _, at, rows in places]
        for (h, at, rows), (out, top, total) in zip(places, strips(items, False)):
            buf[to, at, rows] = (out * (1 / total)).astype(BF)
            lse[side, t, h : h + 1, rows] = top + jnp.log2(total)

    def within(t):
        items = [(buf[Q + t, rows, at], buf[K + t, : rows.stop, at], buf[V + t, : rows.stop, at]) for _, at, rows in places]
        for (h, at, rows), (out, top, total) in zip(places, strips(items, True)):
            far = lse[0, t, h : h + 1, rows]
            high = jnp.maximum(top, far)
            near, far = jnp.exp2(top - high), jnp.exp2(far - high)
            out = (out * near + buf[REM + t, at, rows].astype(F32) * far) * (1 / (total * near + far))
            a[rows, pl.ds(pl.multiple_of(t * TILE + h * HEAD, HEAD), HEAD)] = out.T.astype(BF)

    def half_job(n, _):
        j = n % 2

        @pl.when(n < 2)
        def _():
            w_wait(j)

        @pl.when(n == 2)
        def _():
            for i in range(PARTS):
                a_copy(i).wait_recv()

        rows = pl.ds(pl.multiple_of(((core + n // 2) % 2) * OWN, OWN), OWN)
        acc[j, rows, :] = _dot(a[rows, :HALF], wb[2 * j]) + _dot(a[rows, HALF:], wb[2 * j + 1])

        @pl.when(n == 2)
        def _():
            w_start(2)
            epilogue(0)

            @pl.when(chip == 1)
            def _():
                q_send(0).start()

            @pl.when(first)
            def _():
                k_send.start()

        return 0

    lax.fori_loop(0, 4, half_job, 0)
    acc[0] = acc[1]

    def step(j, _):
        w_wait(j)

        @pl.when(j + 1 < JOBS)
        def _():
            w_start(j + 1)

        @pl.when(j + 1 == JOBS)
        def _():
            o_copy(0).start()
            o_copy(1).start()

        epilogue(j - 1)
        slot = 2 * (j % 2)
        acc[0] = _dot(a[:, :HALF], wb[slot]) + _dot(a[:, HALF:], wb[slot + 1])

        @pl.when((chip == 1) & (j - 1 < LAST))
        def _():
            q_send(j - 1).start()

        @pl.when(first & (j == 2))
        def _():
            v_send.start()

        t = jnp.where(first, jnp.maximum(2 * j - 9, 0) // 5, LAST)

        @pl.when(jnp.where(first, (j >= 5) & ((10 + 5 * t) // 2 == j) & (t < LAST), j == 10))
        def _():
            @pl.when(first)
            def _():
                q_send(t).wait_recv()

            @pl.when(chip == 1)
            def _():
                k_send.wait_recv()
                v_send.wait_recv()

            beyond(t)

            @pl.when(first)
            def _():
                o_send(t).start()
                l_send(t).start()

        return 0

    lax.fori_loop(2, JOBS, step, 0)
    epilogue(JOBS - 1)
    o_copy(2).start()
    o_copy(3).start()

    for i in range(PARTS):
        a_copy(i).wait_send()

    def merge(n, _):
        t = (n + LAST) % TILES

        @pl.when((chip == 1) & (t < LAST))
        def _():
            o_send(t).wait_recv()
            l_send(t).wait_recv()

        within(t)
        return 0

    lax.fori_loop(0, TILES, merge, 0)

    def x_tile(u):
        return pltpu.make_async_copy(x_ref.at[:, pl.ds(pl.multiple_of(u * TILE, TILE), TILE)], xt.at[u % 3], xt_sem.at[u % 3])

    def y_tile(u):
        return pltpu.make_async_copy(yt.at[u % 2], y_ref.at[:, pl.ds(pl.multiple_of(u * TILE, TILE), TILE)], y_sem.at[u % 2])

    def p_send(u):
        return pltpu.make_async_remote_copy(src_ref=acc.at[u % 3, pl.ds(OWN - base, OWN), :], dst_ref=got.at[u], send_sem=ps_sem.at[u % 3],
                                            recv_sem=pr_sem.at[u], device_id=peer, device_id_type=pl.DeviceIdType.MESH)

    def ready(u):
        o_copy(u).wait()
        x_tile(u).start()

        @pl.when((u >= 1) & (u + 3 < OUTS))
        def _():
            o_copy(u + 3).start()

    def project(u):
        sub = (u + 2) % 4
        acc[u % 3] = _dot(a[:, :COLS], wb[sub])

    def finish(u):
        yt[u % 2] = (xt[u % 3].astype(F32) + (acc[u % 3, pl.ds(base, OWN), :] + got[u])).astype(BF)

    def opening(u, _):
        ready(u)
        project(u)
        p_send(u).start()
        return 0

    lax.fori_loop(0, 2, opening, 0)

    def out_step(u, _):
        ready(u)

        @pl.when(u >= 3)
        def _():
            p_send(u - 3).wait_send()

        @pl.when(u >= 4)
        def _():
            y_tile(u - 4).wait()

        p_send(u - 2).wait_recv()
        x_tile(u - 2).wait()
        finish(u - 2)
        project(u)
        p_send(u).start()
        y_tile(u - 2).start()
        return 0

    lax.fori_loop(2, OUTS, out_step, 0)
    for u in (OUTS - 2, OUTS - 1):
        y_tile(u - 2).wait()
        p_send(u).wait_recv()
        x_tile(u).wait()
        finish(u)
        y_tile(u).start()
    for u in range(OUTS - 3, OUTS):
        p_send(u).wait_send()
    for u in (OUTS - 2, OUTS - 1):
        y_tile(u).wait()

    @pl.when(first)
    def _():
        k_send.wait_send()
        v_send.wait_send()

    for t in range(LAST):
        o_send(t).wait_send()

        @pl.when(first)
        def _():
            l_send(t).wait_send()


def solution(mesh):
    def step(x, gain, wq, wk, wv, wo):
        dma = pltpu.SemaphoreType.DMA
        return pl.pallas_call(
            _kernel,
            out_shape=jax.ShapeDtypeStruct((OWN, D), BF),
            in_specs=[pl.BlockSpec(memory_space=pl.ANY), pl.BlockSpec(memory_space=pltpu.VMEM)] + [pl.BlockSpec(memory_space=pl.ANY)] * 4,
            out_specs=pl.BlockSpec(memory_space=pl.ANY),
            scratch_shapes=[
                pltpu.VMEM((ROWS, D), BF),
                pltpu.VMEM((4, HALF, TILE), BF),
                pltpu.VMEM((5 * TILES, ROWS, TILE), BF),
                pltpu.VMEM((2, TILES, 8, ROWS), F32),
                pltpu.VMEM((3, ROWS, TILE), F32),
                pltpu.VMEM((OUTS, OWN, TILE), F32),
                pltpu.VMEM((2, 2, ROWS, HEAD), F32),
                pltpu.VMEM((3, OWN, TILE), BF),
                pltpu.VMEM((2, OWN, TILE), BF),
                dma((PARTS,)), dma((4,)), dma((PARTS,)), dma((PARTS,)),
                dma((TILES + 1,)), dma((TILES,)), dma((TILES + 1,)), dma((TILES,)),
                dma((3,)), dma((OUTS,)), dma((3,)), dma((2,)),
            ],
            compiler_params=pltpu.CompilerParams(collective_id=0, has_side_effects=True, vmem_limit_bytes=67043328),
        )(x, gain, wq, wk, wv, wo)

    tokens, whole = P(("dp", "sp"), None), P(None, None)
    return jax.shard_map(
        step,
        mesh=mesh,
        in_specs=(tokens, P(None), whole, whole, whole, whole),
        out_specs=tokens,
        check_vma=False,
    )
```

```python
import functools
import math

import jax
import jax.numpy as jnp
from jax import lax
from jax.experimental import pallas as pl
from jax.experimental.pallas import tpu as pltpu
from jax.sharding import PartitionSpec as P

HEAD = 128
THETA = 10000
NEG = -1e30
LOG2E = 1.4426950408889634
E2 = HEAD**-0.5 * LOG2E

OWN = 256
ROWS = 2 * OWN
D = 7168
COLS = D // 2
TILE = 512
TILES = COLS // TILE
JOBS = 3 * TILES
HEADS = TILE // HEAD
HALF = D // 2
OUTS = D // TILE
PARTS = 4
PIECE = OWN // PARTS
BF, F32 = jnp.bfloat16, jnp.float32
Q, K, V, REM, OT = (n * TILES for n in range(5))
LAST = TILES - 1


def _dot(a, b):
    return jnp.dot(a, b, preferred_element_type=F32)


def _dotg(a, b, ca, cb):
    return lax.dot_general(a, b, (((ca,), (cb,)), ((), ())), preferred_element_type=F32)


def _kernel(x_ref, gain_ref, wq_ref, wk_ref, wv_ref, wo_ref, y_ref, a, wb, buf, lse, acc, got, tab, xt, yt,
            x_sem, w_sem, as_sem, ar_sem, qs_sem, ls_sem, r_sem, lr_sem, ps_sem, pr_sem, xt_sem, y_sem):
    dp, sp = lax.axis_index("dp"), lax.axis_index("sp")
    chip, core = sp // 2, sp % 2
    peer = (dp, chip * 2 + 1 - core)
    other = (dp, (1 - chip) * 2 + core)
    base = pl.multiple_of(core * OWN, OWN)
    first = chip == 0

    def x_copy(i):
        return pltpu.make_async_copy(x_ref.at[pl.ds(i * PIECE, PIECE), :], a.at[pl.ds(base + i * PIECE, PIECE), :], x_sem.at[i])

    for i in range(PARTS):
        x_copy(i).start()

    lse[0] = jnp.full(lse.shape[1:], NEG, F32)
    lse[1] = jnp.zeros(lse.shape[1:], F32)
    buf[REM + LAST] = jnp.zeros((ROWS, TILE), BF)

    barrier = pltpu.get_barrier_semaphore()
    for who in (peer, other):
        pl.semaphore_signal(barrier, inc=1, device_id=who, device_id_type=pl.DeviceIdType.MESH)

    def job(j):
        early = jnp.where(first, 2 * TILES, TILES)
        n = jnp.where(j < early, j, j - early)
        pairs = (j < early) == first
        return jnp.where(pairs, 1 + n % 2, 0), jnp.where(pairs, (n // 2 + LAST) % TILES, n)

    def w_copy(ref, tile, slot, h):
        cols = pl.ds(pl.multiple_of(core * COLS + tile * TILE, TILE), TILE)
        return pltpu.make_async_copy(ref.at[pl.ds(h * HALF, HALF), cols], wb.at[2 * slot + h], w_sem.at[2 * slot + h])

    def w_piece(ref, tile, slot, h, n):
        cols = pl.ds(pl.multiple_of(core * COLS + tile * TILE, TILE), TILE)
        return pltpu.make_async_copy(ref.at[pl.ds(h * HALF + n * HALF // 2, HALF // 2), cols],
                                     wb.at[2 * slot + h, pl.ds(n * HALF // 2, HALF // 2), :], w_sem.at[2 * slot + h])

    def w_start(j):
        mat, tile = job(j)
        for m, ref in enumerate((wq_ref, wk_ref, wv_ref)):
            @pl.when(mat == m)
            def _():
                for h in range(2):
                    for n in range(2):
                        w_piece(ref, tile, j % 2, h, n).start()

    def w_wait(j):
        for h in range(2):
            w_copy(wq_ref, 0, j % 2, h).wait()

    def o_copy(u):
        rows = pl.ds(pl.multiple_of(core * COLS, COLS), COLS)
        sub = (u + 2) % 4
        return pltpu.make_async_copy(wo_ref.at[rows, pl.ds(pl.multiple_of(u * TILE, TILE), TILE)], wb.at[sub], w_sem.at[sub])

    w_start(0)

    place = (chip * ROWS + lax.broadcasted_iota(jnp.int32, (ROWS, HEAD), 0)).astype(F32)
    lane = lax.broadcasted_iota(jnp.int32, (ROWS, HEAD), 1)
    angle = place * jnp.exp2((lane % 64).astype(F32) * (-math.log2(THETA) / 64))
    tab[0, 0] = jnp.cos(angle)
    sin = jnp.sin(angle)
    tab[0, 1] = jnp.where(lane < 64, -sin, sin)
    tab[1, 0] = jnp.ones((ROWS, HEAD), F32)
    tab[1, 1] = jnp.zeros((ROWS, HEAD), F32)

    def a_copy(i):
        rows = pl.ds(base + i * PIECE, PIECE)
        return pltpu.make_async_remote_copy(src_ref=a.at[rows, :], dst_ref=a.at[rows, :], send_sem=as_sem.at[i], recv_sem=ar_sem.at[i],
                                            device_id=peer, device_id_type=pl.DeviceIdType.MESH)

    gain = gain_ref[...].astype(F32)
    for i in range(PARTS):
        x_copy(i).wait()
        if i == PARTS - 1:
            w_start(1)
        rows = pl.ds(base + i * PIECE, PIECE)
        wide = a[rows, :].astype(F32)
        scale = lax.rsqrt(jnp.mean(wide * wide, -1, keepdims=True) + 1e-6)
        a[rows, :] = (a[rows, :].astype(F32) * scale * gain).astype(BF)
        if i == 1:
            pl.semaphore_wait(barrier, 2)
            a_copy(0).start()
        if i:
            a_copy(i).start()

    def epilogue(j):
        mat, tile = job(j)
        kind = jnp.where(mat == 2, 1, 0)
        cos, sin = tab[kind, 0], tab[kind, 1]
        for h in range(HEADS):
            t = acc[0, :, h * HEAD : (h + 1) * HEAD].astype(BF).astype(F32)
            buf[mat * TILES + tile, :, h * HEAD : (h + 1) * HEAD] = (t * cos + pltpu.roll(t, 64, 1) * sin).astype(BF)

    def move(src, dst, n):
        return pltpu.make_async_remote_copy(src_ref=buf.at[src], dst_ref=buf.at[dst], send_sem=qs_sem.at[n], recv_sem=r_sem.at[n],
                                            device_id=other, device_id_type=pl.DeviceIdType.MESH)

    def q_send(t):
        return move(Q + t, REM + t, t)

    def o_send(t):
        return move(OT + t, REM + t, t)

    k_send, v_send = move(K + LAST, OT, LAST), move(V + LAST, OT + 1, TILES)

    def l_send(t):
        return pltpu.make_async_remote_copy(src_ref=lse.at[1, t], dst_ref=lse.at[0, t], send_sem=ls_sem.at[t], recv_sem=lr_sem.at[t],
                                            device_id=other, device_id_type=pl.DeviceIdType.MESH)

    ones = jnp.ones((8, ROWS), BF)

    def strips(items, mask):
        weights, outs = [], []
        scores = [_dotg(k, q, 1, 1) for q, k, _ in items]
        for s in scores:
            if mask:
                n, m = s.shape
                key, query = (lax.broadcasted_iota(jnp.int32, (m, m), i) for i in range(2))
                cut = jnp.where(key <= query, s[n - m :], 2 * NEG)
                s = cut if n == m else jnp.concatenate([s[: n - m], cut], axis=0)
            top = s.max(axis=0, keepdims=True)
            weights.append((jnp.exp2((s - top) * E2).astype(BF), top * E2))
        for (_, _, v), (p, top) in zip(items, weights):
            mix = _dot(jnp.concatenate([v.T, ones[:, : v.shape[0]]], axis=0), p)
            outs.append((mix[:HEAD], top, mix[HEAD : HEAD + 1]))
        return outs

    places = [(h, slice(h * HEAD, (h + 1) * HEAD), slice(b * OWN, (b + 1) * OWN)) for h in range(HEADS) for b in range(2)]

    def beyond(t):
        q, k, v = jnp.where(first, REM, Q) + t, jnp.where(first, K + t, OT), jnp.where(first, V + t, OT + 1)
        to, side = jnp.where(first, OT, REM) + t, jnp.where(first, 1, 0)
        items = [(buf[q, rows, at], buf[k, :, at], buf[v, :, at]) for _, at, rows in places]
        for (h, at, rows), (out, top, total) in zip(places, strips(items, False)):
            buf[to, at, rows] = (out * (1 / total)).astype(BF)
            lse[side, t, h : h + 1, rows] = top + jnp.log2(total)

    def within(*tiles):
        spots = [(t, *place) for t in tiles for place in places]
        items = [(buf[Q + t, rows, at], buf[K + t, : rows.stop, at], buf[V + t, : rows.stop, at]) for t, _, at, rows in spots]
        for (t, h, at, rows), (out, top, total) in zip(spots, strips(items, True)):
            far = lse[0, t, h : h + 1, rows]
            high = jnp.maximum(top, far)
            near, far = jnp.exp2(top - high), jnp.exp2(far - high)
            out = (out * near + buf[REM + t, at, rows].astype(F32) * far) * (1 / (total * near + far))
            a[rows, pl.ds(pl.multiple_of(t * TILE + h * HEAD, HEAD), HEAD)] = out.T.astype(BF)

    def half_job(n, _):
        j = n % 2

        @pl.when(n < 2)
        def _():
            w_wait(j)

        @pl.when(n == 2)
        def _():
            for i in range(PARTS):
                a_copy(i).wait_recv()

        rows = pl.ds(pl.multiple_of(((core + n // 2) % 2) * OWN, OWN), OWN)
        acc[j, rows, :] = _dot(a[rows, :HALF], wb[2 * j]) + _dot(a[rows, HALF:], wb[2 * j + 1])

        @pl.when(n == 2)
        def _():
            w_start(2)
            epilogue(0)

            @pl.when(chip == 1)
            def _():
                q_send(0).start()

            @pl.when(first)
            def _():
                k_send.start()

        return 0

    lax.fori_loop(0, 4, half_job, 0)
    acc[0] = acc[1]

    def step(j, _):
        w_wait(j)

        @pl.when(j + 1 < JOBS)
        def _():
            w_start(j + 1)

        @pl.when(j + 1 == JOBS)
        def _():
            o_copy(0).start()
            o_copy(1).start()

        epilogue(j - 1)
        slot = 2 * (j % 2)
        acc[0] = _dot(a[:, :HALF], wb[slot]) + _dot(a[:, HALF:], wb[slot + 1])

        @pl.when((chip == 1) & (j - 1 < LAST))
        def _():
            q_send(j - 1).start()

        @pl.when(first & (j == 2))
        def _():
            v_send.start()

        t = jnp.where(first, jnp.maximum(2 * j - 9, 0) // 5, LAST)

        @pl.when(jnp.where(first, (j >= 5) & ((10 + 5 * t) // 2 == j) & (t < LAST), j == 10))
        def _():
            @pl.when(first)
            def _():
                q_send(t).wait_recv()

            @pl.when(chip == 1)
            def _():
                k_send.wait_recv()
                v_send.wait_recv()

            beyond(t)

            @pl.when(first)
            def _():
                o_send(t).start()
                l_send(t).start()

        return 0

    lax.fori_loop(2, JOBS, step, 0)
    epilogue(JOBS - 1)
    o_copy(2).start()
    o_copy(3).start()

    for i in range(PARTS):
        a_copy(i).wait_send()

    within(LAST)

    def merge(n, _):
        pair = 2 * n, 2 * n + 1

        @pl.when(chip == 1)
        def _():
            for t in pair:
                o_send(t).wait_recv()
                l_send(t).wait_recv()

        within(*pair)
        return 0

    lax.fori_loop(0, LAST // 2, merge, 0)

    def x_tile(u):
        return pltpu.make_async_copy(x_ref.at[:, pl.ds(pl.multiple_of(u * TILE, TILE), TILE)], xt.at[u % 3], xt_sem.at[u % 3])

    def y_tile(u):
        return pltpu.make_async_copy(yt.at[u % 2], y_ref.at[:, pl.ds(pl.multiple_of(u * TILE, TILE), TILE)], y_sem.at[u % 2])

    def p_send(u):
        return pltpu.make_async_remote_copy(src_ref=acc.at[u % 3, pl.ds(OWN - base, OWN), :], dst_ref=got.at[u], send_sem=ps_sem.at[u % 3],
                                            recv_sem=pr_sem.at[u], device_id=peer, device_id_type=pl.DeviceIdType.MESH)

    def ready(u):
        o_copy(u).wait()
        x_tile(u).start()

        @pl.when((u >= 1) & (u + 3 < OUTS))
        def _():
            o_copy(u + 3).start()

    def project(u):
        sub = (u + 2) % 4
        acc[u % 3] = _dot(a[:, :COLS], wb[sub])

    def finish(u):
        yt[u % 2] = (xt[u % 3].astype(F32) + (acc[u % 3, pl.ds(base, OWN), :] + got[u])).astype(BF)

    def opening(u, _):
        ready(u)
        project(u)
        p_send(u).start()
        return 0

    lax.fori_loop(0, 2, opening, 0)

    def before(u):
        ready(u)

        @pl.when(u >= 3)
        def _():
            p_send(u - 3).wait_send()

        @pl.when(u >= 4)
        def _():
            y_tile(u - 4).wait()

        p_send(u - 2).wait_recv()
        x_tile(u - 2).wait()

    def out_step(u, _):
        before(u)
        finish(u - 2)
        project(u)
        p_send(u).start()
        y_tile(u - 2).start()
        return 0

    END = OUTS - 1
    lax.fori_loop(2, END, out_step, 0)

    before(END)
    finish(END - 2)
    y_tile(END - 2).start()

    def last_half(n, _):
        rows = pl.ds(pl.multiple_of(((core + 1 + n) % 2) * OWN, OWN), OWN)
        acc[END % 3, rows, :] = _dot(a[rows, :COLS], wb[(END + 2) % 4])

        @pl.when(n == 0)
        def _():
            p_send(END).start()

        return 0

    lax.fori_loop(0, 2, last_half, 0)
    for u in (END - 1, END):
        y_tile(u - 2).wait()
        p_send(u).wait_recv()
        x_tile(u).wait()
        finish(u)
        y_tile(u).start()
    for u in range(OUTS - 3, OUTS):
        p_send(u).wait_send()
    for u in (END - 1, END):
        y_tile(u).wait()

    @pl.when(first)
    def _():
        k_send.wait_send()
        v_send.wait_send()

    for t in range(LAST):
        o_send(t).wait_send()

        @pl.when(first)
        def _():
            l_send(t).wait_send()


def solution(mesh):
    def step(x, gain, wq, wk, wv, wo):
        dma = pltpu.SemaphoreType.DMA
        return pl.pallas_call(
            _kernel,
            out_shape=jax.ShapeDtypeStruct((OWN, D), BF),
            in_specs=[pl.BlockSpec(memory_space=pl.ANY), pl.BlockSpec(memory_space=pltpu.VMEM)] + [pl.BlockSpec(memory_space=pl.ANY)] * 4,
            out_specs=pl.BlockSpec(memory_space=pl.ANY),
            scratch_shapes=[
                pltpu.VMEM((ROWS, D), BF),
                pltpu.VMEM((4, HALF, TILE), BF),
                pltpu.VMEM((5 * TILES, ROWS, TILE), BF),
                pltpu.VMEM((2, TILES, 8, ROWS), F32),
                pltpu.VMEM((3, ROWS, TILE), F32),
                pltpu.VMEM((OUTS, OWN, TILE), F32),
                pltpu.VMEM((2, 2, ROWS, HEAD), F32),
                pltpu.VMEM((3, OWN, TILE), BF),
                pltpu.VMEM((2, OWN, TILE), BF),
                dma((PARTS,)), dma((4,)), dma((PARTS,)), dma((PARTS,)),
                dma((TILES + 1,)), dma((TILES,)), dma((TILES + 1,)), dma((TILES,)),
                dma((3,)), dma((OUTS,)), dma((3,)), dma((2,)),
            ],
            compiler_params=pltpu.CompilerParams(collective_id=0, has_side_effects=True, vmem_limit_bytes=67043328),
        )(x, gain, wq, wk, wv, wo)

    tokens, whole = P(("dp", "sp"), None), P(None, None)
    return jax.shard_map(
        step,
        mesh=mesh,
        in_specs=(tokens, P(None), whole, whole, whole, whole),
        out_specs=tokens,
        check_vma=False,
    )
```

```python
import functools
import math

import jax
import jax.numpy as jnp
from jax import lax
from jax.experimental import pallas as pl
from jax.experimental.pallas import tpu as pltpu
from jax.sharding import PartitionSpec as P

HEAD = 128
THETA = 10000
NEG = -1e30
LOG2E = 1.4426950408889634
E2 = HEAD**-0.5 * LOG2E

OWN = 256
ROWS = 2 * OWN
D = 7168
COLS = D // 2
TILE = 512
TILES = COLS // TILE
JOBS = 3 * TILES
HEADS = TILE // HEAD
HALF = D // 2
OUTS = D // TILE
PARTS = 4
PIECE = OWN // PARTS
BF, F32 = jnp.bfloat16, jnp.float32
Q, K, V, REM, OT = (n * TILES for n in range(5))
LAST = TILES - 1


def _dot(a, b):
    return jnp.dot(a, b, preferred_element_type=F32)


def _dotg(a, b, ca, cb):
    return lax.dot_general(a, b, (((ca,), (cb,)), ((), ())), preferred_element_type=F32)


def _kernel(x_ref, gain_ref, wq_ref, wk_ref, wv_ref, wo_ref, y_ref, a, wb, buf, lse, acc, got, tab, xt, yt,
            x_sem, w_sem, as_sem, ar_sem, qs_sem, ls_sem, r_sem, lr_sem, ps_sem, pr_sem, xt_sem, y_sem):
    dp, sp = lax.axis_index("dp"), lax.axis_index("sp")
    chip, core = sp // 2, sp % 2
    peer = (dp, chip * 2 + 1 - core)
    other = (dp, (1 - chip) * 2 + core)
    base = pl.multiple_of(core * OWN, OWN)
    first = chip == 0

    def x_copy(i):
        return pltpu.make_async_copy(x_ref.at[pl.ds(i * PIECE, PIECE), :], a.at[pl.ds(base + i * PIECE, PIECE), :], x_sem.at[i])

    for i in range(PARTS):
        x_copy(i).start()

    lse[0] = jnp.full(lse.shape[1:], NEG, F32)
    lse[1] = jnp.zeros(lse.shape[1:], F32)
    buf[REM + LAST] = jnp.zeros((ROWS, TILE), BF)

    barrier = pltpu.get_barrier_semaphore()
    for who in (peer, other):
        pl.semaphore_signal(barrier, inc=1, device_id=who, device_id_type=pl.DeviceIdType.MESH)

    def job(j):
        early = jnp.where(first, 2 * TILES, TILES)
        n = jnp.where(j < early, j, j - early)
        pairs = (j < early) == first
        return jnp.where(pairs, 1 + n % 2, 0), jnp.where(pairs, (n // 2 + LAST) % TILES, n)

    def w_copy(ref, tile, slot, h):
        cols = pl.ds(pl.multiple_of(core * COLS + tile * TILE, TILE), TILE)
        return pltpu.make_async_copy(ref.at[pl.ds(h * HALF, HALF), cols], wb.at[2 * slot + h], w_sem.at[2 * slot + h])

    def w_piece(ref, tile, slot, h, n):
        cols = pl.ds(pl.multiple_of(core * COLS + tile * TILE, TILE), TILE)
        return pltpu.make_async_copy(ref.at[pl.ds(h * HALF + n * HALF // 2, HALF // 2), cols],
                                     wb.at[2 * slot + h, pl.ds(n * HALF // 2, HALF // 2), :], w_sem.at[2 * slot + h])

    def w_start(j):
        mat, tile = job(j)
        for m, ref in enumerate((wq_ref, wk_ref, wv_ref)):
            @pl.when(mat == m)
            def _():
                for h in range(2):
                    for n in range(2):
                        w_piece(ref, tile, j % 2, h, n).start()

    def w_wait(j):
        for h in range(2):
            w_copy(wq_ref, 0, j % 2, h).wait()

    def o_copy(u):
        rows = pl.ds(pl.multiple_of(core * COLS, COLS), COLS)
        sub = (u + 2) % 4
        return pltpu.make_async_copy(wo_ref.at[rows, pl.ds(pl.multiple_of(u * TILE, TILE), TILE)], wb.at[sub], w_sem.at[sub])

    w_start(0)

    place = (chip * ROWS + lax.broadcasted_iota(jnp.int32, (ROWS, HEAD), 0)).astype(F32)
    lane = lax.broadcasted_iota(jnp.int32, (ROWS, HEAD), 1)
    angle = place * jnp.exp2((lane % 64).astype(F32) * (-math.log2(THETA) / 64))
    tab[0, 0] = jnp.cos(angle)
    sin = jnp.sin(angle)
    tab[0, 1] = jnp.where(lane < 64, -sin, sin)
    tab[1, 0] = jnp.ones((ROWS, HEAD), F32)
    tab[1, 1] = jnp.zeros((ROWS, HEAD), F32)

    def a_copy(i):
        rows = pl.ds(base + i * PIECE, PIECE)
        return pltpu.make_async_remote_copy(src_ref=a.at[rows, :], dst_ref=a.at[rows, :], send_sem=as_sem.at[i], recv_sem=ar_sem.at[i],
                                            device_id=peer, device_id_type=pl.DeviceIdType.MESH)

    gain = gain_ref[...].astype(F32)
    for i in range(PARTS):
        x_copy(i).wait()
        if i == PARTS - 1:
            w_start(1)
        rows = pl.ds(base + i * PIECE, PIECE)
        wide = a[rows, :].astype(F32)
        scale = lax.rsqrt(jnp.mean(wide * wide, -1, keepdims=True) + 1e-6)
        a[rows, :] = (a[rows, :].astype(F32) * scale * gain).astype(BF)
        if i == 1:
            pl.semaphore_wait(barrier, 2)
            a_copy(0).start()
        if i:
            a_copy(i).start()

    def epilogue(j):
        mat, tile = job(j)
        kind = jnp.where(mat == 2, 1, 0)
        cos, sin = tab[kind, 0], tab[kind, 1]
        for h in range(HEADS):
            t = acc[0, :, h * HEAD : (h + 1) * HEAD].astype(BF).astype(F32)
            buf[mat * TILES + tile, :, h * HEAD : (h + 1) * HEAD] = (t * cos + pltpu.roll(t, 64, 1) * sin).astype(BF)

    def move(src, dst, n):
        return pltpu.make_async_remote_copy(src_ref=buf.at[src], dst_ref=buf.at[dst], send_sem=qs_sem.at[n], recv_sem=r_sem.at[n],
                                            device_id=other, device_id_type=pl.DeviceIdType.MESH)

    def q_send(t):
        return move(Q + t, REM + t, t)

    def o_send(t):
        return move(OT + t, REM + t, t)

    k_send, v_send = move(K + LAST, OT, LAST), move(V + LAST, OT + 1, TILES)

    def l_send(t):
        return pltpu.make_async_remote_copy(src_ref=lse.at[1, t], dst_ref=lse.at[0, t], send_sem=ls_sem.at[t], recv_sem=lr_sem.at[t],
                                            device_id=other, device_id_type=pl.DeviceIdType.MESH)

    ones = jnp.ones((8, ROWS), BF)

    def strips(items, mask):
        weights, outs = [], []
        scores = [_dotg(k, q, 1, 1) for q, k, _ in items]
        for s in scores:
            if mask:
                n, m = s.shape
                key, query = (lax.broadcasted_iota(jnp.int32, (m, m), i) for i in range(2))
                cut = jnp.where(key <= query, s[n - m :], 2 * NEG)
                s = cut if n == m else jnp.concatenate([s[: n - m], cut], axis=0)
            top = s.max(axis=0, keepdims=True)
            weights.append((jnp.exp2((s - top) * E2).astype(BF), top * E2))
        for (_, _, v), (p, top) in zip(items, weights):
            mix = _dot(jnp.concatenate([v.T, ones[:, : v.shape[0]]], axis=0), p)
            outs.append((mix[:HEAD], top, mix[HEAD : HEAD + 1]))
        return outs

    places = [(h, slice(h * HEAD, (h + 1) * HEAD), slice(b * OWN, (b + 1) * OWN)) for h in range(HEADS) for b in range(2)]

    def beyond(t):
        q, k, v = jnp.where(first, REM, Q) + t, jnp.where(first, K + t, OT), jnp.where(first, V + t, OT + 1)
        to, side = jnp.where(first, OT, REM) + t, jnp.where(first, 1, 0)
        items = [(buf[q, rows, at], buf[k, :, at], buf[v, :, at]) for _, at, rows in places]
        for (h, at, rows), (out, top, total) in zip(places, strips(items, False)):
            buf[to, at, rows] = (out * (1 / total)).astype(BF)
            lse[side, t, h : h + 1, rows] = top + jnp.log2(total)

    def within(*tiles):
        spots = [(t, *place) for t in tiles for place in places]
        items = [(buf[Q + t, rows, at], buf[K + t, : rows.stop, at], buf[V + t, : rows.stop, at]) for t, _, at, rows in spots]
        for (t, h, at, rows), (out, top, total) in zip(spots, strips(items, True)):
            far = lse[0, t, h : h + 1, rows]
            high = jnp.maximum(top, far)
            near, far = jnp.exp2(top - high), jnp.exp2(far - high)
            out = (out * near + buf[REM + t, at, rows].astype(F32) * far) * (1 / (total * near + far))
            a[rows, pl.ds(pl.multiple_of(t * TILE + h * HEAD, HEAD), HEAD)] = out.T.astype(BF)

    def half_job(n, _):
        j = n % 2

        @pl.when(n < 2)
        def _():
            w_wait(j)

        @pl.when(n == 2)
        def _():
            for i in range(PARTS):
                a_copy(i).wait_recv()

        rows = pl.ds(pl.multiple_of(((core + n // 2) % 2) * OWN, OWN), OWN)
        acc[j, rows, :] = _dot(a[rows, :HALF], wb[2 * j]) + _dot(a[rows, HALF:], wb[2 * j + 1])

        @pl.when(n == 2)
        def _():
            w_start(2)
            epilogue(0)

            @pl.when(chip == 1)
            def _():
                q_send(0).start()

            @pl.when(first)
            def _():
                k_send.start()

        return 0

    lax.fori_loop(0, 4, half_job, 0)
    acc[0] = acc[1]

    def step(j, _):
        w_wait(j)

        @pl.when(j + 1 < JOBS)
        def _():
            w_start(j + 1)

        @pl.when(j + 1 == JOBS)
        def _():
            o_copy(0).start()
            o_copy(1).start()

        epilogue(j - 1)
        slot = 2 * (j % 2)
        acc[0] = _dot(a[:, :HALF], wb[slot]) + _dot(a[:, HALF:], wb[slot + 1])

        @pl.when((chip == 1) & (j - 1 < LAST))
        def _():
            q_send(j - 1).start()

        @pl.when(first & (j == 2))
        def _():
            v_send.start()

        t = jnp.where(first, jnp.maximum(2 * j - 9, 0) // 5, LAST)

        @pl.when(jnp.where(first, (j >= 5) & ((10 + 5 * t) // 2 == j) & (t < LAST), j == 10))
        def _():
            @pl.when(first)
            def _():
                q_send(t).wait_recv()

            @pl.when(chip == 1)
            def _():
                k_send.wait_recv()
                v_send.wait_recv()

            beyond(t)

            @pl.when(first)
            def _():
                o_send(t).start()
                l_send(t).start()

        return 0

    lax.fori_loop(2, JOBS, step, 0)
    epilogue(JOBS - 1)
    o_copy(2).start()
    o_copy(3).start()

    for i in range(PARTS):
        a_copy(i).wait_send()

    within(LAST)

    def merge(n, _):
        pair = 2 * n, 2 * n + 1

        @pl.when(chip == 1)
        def _():
            for t in pair:
                o_send(t).wait_recv()
                l_send(t).wait_recv()

        within(*pair)
        return 0

    lax.fori_loop(0, LAST // 2, merge, 0)

    def x_tile(u):
        return pltpu.make_async_copy(x_ref.at[:, pl.ds(pl.multiple_of(u * TILE, TILE), TILE)], xt.at[u % 3], xt_sem.at[u % 3])

    def y_tile(u):
        return pltpu.make_async_copy(yt.at[u % 2], y_ref.at[:, pl.ds(pl.multiple_of(u * TILE, TILE), TILE)], y_sem.at[u % 2])

    def p_send(u):
        return pltpu.make_async_remote_copy(src_ref=acc.at[u % 3, pl.ds(OWN - base, OWN), :], dst_ref=got.at[u], send_sem=ps_sem.at[u % 3],
                                            recv_sem=pr_sem.at[u], device_id=peer, device_id_type=pl.DeviceIdType.MESH)

    def ready(u):
        o_copy(u).wait()
        x_tile(u).start()

        @pl.when((u >= 1) & (u + 3 < OUTS))
        def _():
            o_copy(u + 3).start()

    def project(u):
        sub = (u + 2) % 4
        acc[u % 3] = _dot(a[:, :COLS], wb[sub])

    def finish(u):
        yt[u % 2] = (xt[u % 3].astype(F32) + (acc[u % 3, pl.ds(base, OWN), :] + got[u])).astype(BF)

    def opening(u, _):
        ready(u)
        project(u)
        p_send(u).start()
        return 0

    lax.fori_loop(0, 2, opening, 0)

    def before(u):
        ready(u)

        @pl.when(u >= 3)
        def _():
            p_send(u - 3).wait_send()

        @pl.when(u >= 4)
        def _():
            y_tile(u - 4).wait()

        p_send(u - 2).wait_recv()
        x_tile(u - 2).wait()

    def out_step(u, _):
        before(u)
        finish(u - 2)
        project(u)
        p_send(u).start()
        y_tile(u - 2).start()
        return 0

    END = OUTS - 1
    lax.fori_loop(2, END, out_step, 0)

    before(END)
    finish(END - 2)
    y_tile(END - 2).start()

    def last_half(n, _):
        rows = pl.ds(pl.multiple_of(((core + 1 + n) % 2) * OWN, OWN), OWN)
        acc[END % 3, rows, :] = _dot(a[rows, :COLS], wb[(END + 2) % 4])

        @pl.when(n == 0)
        def _():
            p_send(END).start()

        return 0

    lax.fori_loop(0, 2, last_half, 0)
    for u in (END - 1, END):
        y_tile(u - 2).wait()
        p_send(u).wait_recv()
        x_tile(u).wait()
        finish(u)
        y_tile(u).start()
    for u in range(OUTS - 3, OUTS):
        p_send(u).wait_send()
    for u in (END - 1, END):
        y_tile(u).wait()

    @pl.when(first)
    def _():
        k_send.wait_send()
        v_send.wait_send()

    for t in range(LAST):
        o_send(t).wait_send()

        @pl.when(first)
        def _():
            l_send(t).wait_send()


def _hand_on(y_ref, o_ref, held, in_sem, out_sem):
    n = held.shape[0]
    rows = OWN // n
    ins = [pltpu.make_async_copy(y_ref.at[pl.ds(i * rows, rows), :], held.at[i], in_sem.at[i]) for i in range(n)]
    outs = [pltpu.make_async_copy(held.at[i], o_ref.at[pl.ds(i * rows, rows), :], out_sem.at[i]) for i in range(n)]
    for c in ins:
        c.start()
    for c, o in zip(ins, outs):
        c.wait()
        o.start()
    for o in outs:
        o.wait()


def solution(mesh):
    def step(x, gain, wq, wk, wv, wo):
        dma = pltpu.SemaphoreType.DMA
        y = pl.pallas_call(
            _kernel,
            out_shape=jax.ShapeDtypeStruct((OWN, D), BF),
            in_specs=[pl.BlockSpec(memory_space=pl.ANY), pl.BlockSpec(memory_space=pltpu.VMEM)] + [pl.BlockSpec(memory_space=pl.ANY)] * 4,
            out_specs=pl.BlockSpec(memory_space=pl.ANY),
            scratch_shapes=[
                pltpu.VMEM((ROWS, D), BF),
                pltpu.VMEM((4, HALF, TILE), BF),
                pltpu.VMEM((5 * TILES, ROWS, TILE), BF),
                pltpu.VMEM((2, TILES, 8, ROWS), F32),
                pltpu.VMEM((3, ROWS, TILE), F32),
                pltpu.VMEM((OUTS, OWN, TILE), F32),
                pltpu.VMEM((2, 2, ROWS, HEAD), F32),
                pltpu.VMEM((3, OWN, TILE), BF),
                pltpu.VMEM((2, OWN, TILE), BF),
                dma((PARTS,)), dma((4,)), dma((PARTS,)), dma((PARTS,)),
                dma((TILES + 1,)), dma((TILES,)), dma((TILES + 1,)), dma((TILES,)),
                dma((3,)), dma((OUTS,)), dma((3,)), dma((2,)),
            ],
            compiler_params=pltpu.CompilerParams(collective_id=0, has_side_effects=True, vmem_limit_bytes=67043328),
        )(x, gain, wq, wk, wv, wo)
        return pl.pallas_call(
            _hand_on,
            out_shape=jax.ShapeDtypeStruct((OWN, D), BF),
            in_specs=[pl.BlockSpec(memory_space=pl.ANY)],
            out_specs=pl.BlockSpec(memory_space=pl.ANY),
            scratch_shapes=[pltpu.VMEM((8, OWN // 8, D), BF), dma((8,)), dma((8,))],
            compiler_params=pltpu.CompilerParams(vmem_limit_bytes=67043328),
        )(y)

    tokens, whole = P(("dp", "sp"), None), P(None, None)
    return jax.shard_map(
        step,
        mesh=mesh,
        in_specs=(tokens, P(None), whole, whole, whole, whole),
        out_specs=tokens,
        check_vma=False,
    )
```
